32 devices in a mesh: dp: 4 (over y, x), expert: 8 (over z, core).
Axes of the slice: x: 2, y: 2, z: 4, core: 2. Of those that a mesh axis runs over, the one named last changes fastest.
Arguments:
- grad_out: bfloat16 [4096, 3072], P(('dp', 'expert')), may hold values from -6 to 6
- expert_ids: int32 [4096, 2], P(('dp', 'expert')), may hold values from 0 to 7, all different within a row; in each aligned block of 128 rows (0 to 127, 128 to 255, ...) at most 36 rows name the same one
- down_weight: bfloat16 [8, 1024, 3072], P('expert'), may hold values from -0.109375 to 0.109375
- history_grad: float32 [8, 8], replicated, may hold values from 0.5 to 3
- history_hidden: float32 [8, 8], replicated, may hold values from 0.5 to 3
Outputs:
- hidden_scaled: bfloat16 [4, 8, 288, 1024], P('dp', 'expert')
- new_history_grad: float32 [8, 8], replicated
- new_history_hidden: float32 [8, 8], replicated
The draws below stay inside these ranges and needn't reach their ends.
Inputs may be any that keep to these rules, and one draw needn't show every extreme that they name: `expert_ids`: each row names 2 different experts; among the 128 rows of one device no expert is named more than 36 times, a bound that some block reaches in some devices.
All inputs are finite; a program needn't handle non-finite values.
Results may differ from the reference program's by a relative error of at most 0.0045.
Values may be sent and summed in bfloat16 or wider, within the bound.
No kernel may reach another device: no remote copies, remote signals or barrier semaphores. Data moves between devices by JAX's collectives and lax.ppermute only.
A program may use at most 128 MiB of HBM per device.

```python
import math
import jax
import jax.numpy as jnp
import numpy as np
from jax import lax

D = 3072
EXPERTS = 8
TOP = 2
FF_DEV = 1024
HIST = 8
TOK_DEV = 128
CAP = 36
TOKENS = 4096
N_DP = 4
N_EXPERT = 8


def steps_of(key, dims, split, smallest, top_value):
    level, own = 1.0, jax.random.fold_in(key, 6)
    for axis_at, shards_of in split:
        steps = jnp.exp(jax.random.uniform(jax.random.fold_in(own, axis_at), (shards_of,), jnp.float32, smallest / len(split), top_value / len(split)))
        level = level * jnp.repeat(steps, dims[axis_at] // shards_of).reshape([-1 if axis == axis_at else 1 for axis in range(len(dims))])
    return level


def deal_out(own_key, own, number, rows, number_of, top, bound, lean):
    ranking = jax.random.permutation(own_key, number_of)
    packed, ordinary = portions_of(number_of, rows * top, bound, lean, True), portions_of(number_of, rows * top, bound, lean, False)
    places = jnp.arange(number_of)

    def named(lengths, turn):
        used = int((lengths > 0).sum())
        fixed = max(1, used // 4)
        moved = fixed + (places - fixed + turn * (used - fixed)) % max(1, number_of - fixed)
        return jnp.zeros((number_of,), jnp.int32).at[ranking[jnp.where(places < fixed, places, moved)]].set(jnp.asarray(lengths, jnp.int32))

    lengths = jnp.where(number % 4 == 0, named(packed, number // 4), named(ordinary, number - number // 4 - 1))
    mixed = jax.random.permutation(jax.random.fold_in(own, 3), number_of)
    giver, receiver = mixed[0:number_of // 2 * 2:2], mixed[1:number_of // 2 * 2:2]
    room = jnp.minimum(lengths[giver] - 1, bound - lengths[receiver]) // 2
    room = jnp.where((giver == ranking[0]) | (receiver == ranking[0]) | (lengths[receiver] == 0), 0, jnp.maximum(room, 0))
    moved = jax.random.randint(jax.random.fold_in(own, 4), (number_of // 2,), 0, 1 << 20) % (room + 1)
    lengths = lengths.at[giver].add(-moved).at[receiver].add(moved)
    items = jnp.searchsorted(jnp.cumsum(lengths), jnp.arange(rows * top), side="right").astype(jnp.int32)
    grid = items.reshape(top, rows).T
    grid = grid[jax.random.permutation(jax.random.fold_in(own, 1), rows)]
    turn = jax.random.randint(jax.random.fold_in(own, 2), (rows, 1), 0, top)
    return jnp.take_along_axis(grid, (jnp.arange(top)[None, :] + turn) % top, axis=1)


def portions_of(count, total, bound, slope, full):
    loads = [(1 << 20) // math.isqrt(rank ** slope) + 1 for rank in range(1, count + 1)]
    largest = bound if full else min(bound, max(-(-total // count), total * loads[0] // sum(loads)))
    least = 1 if total - largest >= count - 1 else 0
    given, surplus = [largest] + [least] * (count - 1), total - largest - least * (count - 1)
    while surplus > 0:
        candidates = [i for i in range(1, count) if given[i] < largest] or [i for i in range(1, count) if given[i] < bound]
        mass, budget = sum([loads[i] for i in candidates]), surplus
        for i in candidates:
            extra = min(bound - given[i], max(1, budget * loads[i] // mass), surplus)
            given[i] = given[i] + extra
            surplus = surplus - extra
    return np.array(given)


def centred(own_key, shape, spread, bound, split=(), held_as=jnp.bfloat16):
    result = jax.random.normal(own_key, shape, jnp.float32) * spread
    if len(split) > 0:
        result = steps_of(own_key, shape, split, -0.22, 0.18) * result
    return jnp.clip(result, min=-bound, max=bound).astype(held_as)


def setup_inputs(seed: int = 0) -> dict:
    seeds = jax.random.split(jax.random.key(seed), 6)
    grad_out = centred(seeds[0], (TOKENS, D), 1.0, 6.0, ((0, 32),))
    expert_ids_keys = jax.random.split(jax.random.fold_in(seeds[1], 1), TOKENS // TOK_DEV)
    expert_ids_turns = jax.random.permutation(jax.random.fold_in(seeds[1], 3), TOKENS // TOK_DEV)
    expert_ids = jax.vmap(lambda own, number: deal_out(jax.random.fold_in(seeds[1], 2), own, number, TOK_DEV, EXPERTS, TOP, CAP, 2))(expert_ids_keys, expert_ids_turns).reshape((TOKENS, TOP))
    down_weight = centred(seeds[2], (N_EXPERT, FF_DEV, D), D ** -0.5, 0.109375, ((0, 8),))
    history_grad = jnp.clip(jnp.exp(jax.random.uniform(seeds[3], (HIST, EXPERTS), jnp.float32, math.log(0.5), math.log(3.0))), 0.5, 3.0)
    history_hidden = jnp.clip(jnp.exp(jax.random.uniform(seeds[4], (HIST, EXPERTS), jnp.float32, math.log(0.5), math.log(3.0))), 0.5, 3.0)
    return {"grad_out": grad_out, "expert_ids": expert_ids, "down_weight": down_weight, "history_grad": history_grad, "history_hidden": history_hidden}


def reference(grad_out, expert_ids, down_weight, history_grad, history_hidden):
    slices = N_EXPERT // EXPERTS
    routing = expert_ids.reshape(N_DP, N_EXPERT, TOK_DEV * TOP)
    onehot = (routing[..., None] == jnp.arange(EXPERTS, dtype=jnp.int32)).astype(jnp.int32)
    before = jnp.cumsum(onehot, axis=2) - onehot
    slot_index = jnp.sum(before * onehot, axis=-1).astype(jnp.int32)
    scale_in = 1.0 / jnp.max(history_grad, axis=0)
    scale_hidden = 1.0 / jnp.max(history_hidden, axis=0)
    gradients = grad_out.reshape(N_DP, N_EXPERT, TOK_DEV, D)
    row_peak = jnp.max(jnp.abs(gradients.astype(jnp.float32)), axis=-1)
    routed = jnp.max(onehot.reshape(N_DP, N_EXPERT, TOK_DEV, TOP, EXPERTS), axis=3) > 0
    grad_amax = jnp.max(jnp.where(routed, row_peak[..., None], 0.0), axis=(0, 1, 2))
    token_of = jnp.arange(TOK_DEV * TOP, dtype=jnp.int32) // TOP
    weights = down_weight.reshape(EXPERTS, slices * FF_DEV, D)
    source_index = jnp.broadcast_to(jnp.arange(N_EXPERT, dtype=jnp.int32)[:, None], (N_EXPERT, TOK_DEV * TOP))

    def one_replica(inputs):
        grads_here, routing_here, slots_here = inputs
        token_rows = grads_here[:, token_of].astype(jnp.float32)
        quantized = jnp.clip(token_rows * scale_in[routing_here][..., None], -1.0, 1.0).astype(jnp.bfloat16)
        buffer = jnp.zeros((EXPERTS, N_EXPERT, CAP, D), jnp.bfloat16)
        buffer = buffer.at[routing_here, source_index, slots_here].set(quantized)

        def one_expert(pair):
            expert, block = pair
            received = block.reshape(N_EXPERT * CAP, D)
            product = jnp.dot(received, weights[expert].T, preferred_element_type=jnp.float32)
            hidden = product / scale_in[expert]
            scaled = jnp.clip(hidden * scale_hidden[expert], -1.0, 1.0).astype(jnp.bfloat16)
            scaled = scaled.reshape(N_EXPERT * CAP, slices, FF_DEV).transpose(1, 0, 2)
            return scaled, jnp.max(jnp.abs(hidden))

        scaled, peak_values = lax.map(one_expert, (jnp.arange(EXPERTS, dtype=jnp.int32), buffer))
        return scaled.reshape(N_EXPERT, N_EXPERT * CAP, FF_DEV), peak_values

    hidden_scaled, peak_values = lax.map(one_replica, (gradients, routing, slot_index))
    hidden_amax = jnp.max(peak_values, axis=0)
    new_history_grad = jnp.concatenate([history_grad[1:], grad_amax[None, :]], axis=0)
    new_history_hidden = jnp.concatenate([history_hidden[1:], hidden_amax[None, :]], axis=0)
    return hidden_scaled, new_history_grad, new_history_hidden
```

```python
import functools

import jax
import jax.numpy as jnp
from jax import lax
from jax.experimental import pallas as pl
from jax.experimental.pallas import tpu as pltpu
from jax.sharding import PartitionSpec as P

VMEM = pl.BlockSpec(memory_space=pltpu.VMEM)


def choice_map(ids, order, experts):
    return (ids[0:1, :] == order) | (ids[1:2, :] == order)


def pick(values, index):
    lanes = lax.broadcasted_iota(jnp.int32, values.shape, 1)
    return jnp.sum(jnp.where(lanes == index, values, 0.0), axis=1, keepdims=True)


def dispatch_kernel(experts, capacity, ids_ref, grad_ref, history_ref, *out_refs):
    tokens, features = grad_ref.shape
    half = features // 2
    me = lax.axis_index("expert")
    ids = ids_ref[...]
    order = lax.broadcasted_iota(jnp.int32, (experts, tokens), 0) ^ me
    named = choice_map(ids, order, experts)
    before = (
        lax.broadcasted_iota(jnp.int32, (tokens, tokens), 0)
        < lax.broadcasted_iota(jnp.int32, (tokens, tokens), 1)
    )
    slot = jnp.dot(
        jnp.where(named, 1.0, 0.0).astype(jnp.bfloat16),
        jnp.where(before, 1.0, 0.0).astype(jnp.bfloat16),
        preferred_element_type=jnp.float32,
    ).astype(jnp.int32)
    slot = jnp.where(named, slot, -1 - 2 * capacity)
    scale = 1.0 / jnp.max(history_ref[...], axis=0, keepdims=True)
    rows = lax.broadcasted_iota(jnp.int32, (2 * capacity, tokens), 0)
    stacked = jnp.concatenate([grad_ref[:, :half], grad_ref[:, half:]], axis=0)
    for k in range(experts):
        mine = slot[k : k + 1, :]
        top = jnp.where(mine == rows, 1.0, 0.0)
        bottom = jnp.where(mine == rows - capacity, 1.0, 0.0)
        select = jnp.concatenate([top, bottom], axis=1).astype(jnp.bfloat16)
        rowsum = jnp.dot(select, stacked, preferred_element_type=jnp.float32)
        factor = pick(scale, me ^ k)
        out_refs[k][...] = jnp.clip(rowsum * factor, -1.0, 1.0).astype(jnp.bfloat16)


def project(blocks, capacity, weight_ref, history_grad_ref, history_hidden_ref, low_ref, high_ref, pair_refs):
    me = lax.axis_index("expert")
    part = blocks[0].shape[0] // 2 + 4
    offset = 2 * capacity - part
    half = weight_ref.shape[1] // 2
    for i, block in enumerate(blocks):
        low_ref[i * part : (i + 1) * part, :] = block[0:part, :]
        high_ref[i * part : (i + 1) * part, :] = block[offset:, :]
    contract = (((1,), (1,)), ((), ()))
    low = lax.dot_general(
        low_ref[...], weight_ref[:, :half], contract, preferred_element_type=jnp.float32
    )
    high = lax.dot_general(
        high_ref[...], weight_ref[:, half:], contract, preferred_element_type=jnp.float32
    )
    skip = capacity - offset
    products = [
        low[i * part : i * part + capacity] + high[i * part + skip : i * part + skip + capacity]
        for i in range(len(blocks))
    ]
    scale_in = pick(1.0 / jnp.max(history_grad_ref[...], axis=0, keepdims=True), me)
    scale_hidden = pick(1.0 / jnp.max(history_hidden_ref[...], axis=0, keepdims=True), me)
    restore = 1.0 / scale_in
    peak = functools.reduce(jnp.maximum, [jnp.abs(p) for p in products])
    peak = jnp.max(jnp.max(peak, axis=0, keepdims=True), axis=1, keepdims=True) * restore
    first_core = (me & 1) == 0
    for j, ref in enumerate(pair_refs):
        a = jnp.clip(products[2 * j] * restore * scale_hidden, -1.0, 1.0)
        b = jnp.clip(products[2 * j + 1] * restore * scale_hidden, -1.0, 1.0)
        top, bottom = jnp.where(first_core, a, b), jnp.where(first_core, b, a)
        ref[...] = jnp.concatenate([top, bottom], axis=0).astype(jnp.bfloat16)
    return peak


def early_kernel(experts, capacity, count, *refs):
    blocks = refs[:count]
    weight_ref, history_grad_ref, history_hidden_ref, ids_ref, grad_ref = refs[count : count + 5]
    outs = refs[count + 5 : -2]
    low_ref, high_ref = refs[-2:]
    me = lax.axis_index("expert")
    peak = project(
        blocks, capacity, weight_ref, history_grad_ref, history_hidden_ref, low_ref, high_ref, outs[:-1]
    )
    tokens = grad_ref.shape[0]
    order = lax.broadcasted_iota(jnp.int32, (experts, tokens), 0)
    named = choice_map(ids_ref[...], order, experts)
    row_peak = jnp.max(jnp.abs(grad_ref[...].astype(jnp.float32)), axis=1, keepdims=True)
    row_peak = jnp.broadcast_to(row_peak, (tokens, tokens)).T[0:1, :]
    grad_peak = jnp.max(jnp.where(named, row_peak, 0.0), axis=1, keepdims=True)
    lanes = lax.broadcasted_iota(jnp.int32, (experts, 128), 1)
    spread = jnp.where(
        lanes == lax.broadcasted_iota(jnp.int32, (experts, 128), 0), grad_peak, 0.0
    )
    vector = jnp.max(spread, axis=0, keepdims=True)
    lane = lax.broadcasted_iota(jnp.int32, (1, 128), 1)
    outs[-1][...] = jnp.where(lane == experts + me, peak, vector)


def late_kernel(experts, capacity, count, *refs):
    blocks = refs[:count]
    weight_ref, history_grad_ref, history_hidden_ref, vector_ref = refs[count : count + 4]
    outs = refs[count + 4 : -2]
    low_ref, high_ref = refs[-2:]
    me = lax.axis_index("expert")
    peak = project(
        blocks, capacity, weight_ref, history_grad_ref, history_hidden_ref, low_ref, high_ref, outs[:-1]
    )
    lane = lax.broadcasted_iota(jnp.int32, (1, 128), 1)
    vector = jnp.maximum(vector_ref[...], jnp.where(lane == experts + me, peak, 0.0))
    outs[-1][...] = jnp.broadcast_to(vector, outs[-1].shape)


def assemble_kernel(capacity, *refs):
    pairs, out_ref = refs[:-1], refs[-1]
    chip = lax.axis_index("expert") // 2
    for j, ref in enumerate(pairs):
        start = pl.multiple_of((chip ^ j) * 2 * capacity, 8)
        out_ref[pl.ds(start, 2 * capacity), :] = ref[...]


def finish_kernel(experts, peaks_ref, history_grad_ref, history_hidden_ref, grad_out_ref, hidden_out_ref):
    peaks = jnp.max(peaks_ref[...], axis=0, keepdims=True)
    history = history_grad_ref.shape[0]
    for ref, out, at in (
        (history_grad_ref, grad_out_ref, 0),
        (history_hidden_ref, hidden_out_ref, experts),
    ):
        out[0 : history - 1, :] = ref[1:history, :]
        out[history - 1 : history, :] = peaks[:, at : at + experts]


def fast_device(grad_out, expert_ids, down_weight, history_grad, history_hidden):
    tokens, features = grad_out.shape
    experts = history_grad.shape[1]
    capacity = tokens * 9 // 32
    units = down_weight.shape[1]
    half = experts // 2
    devices = lax.axis_size("dp") * lax.axis_size("expert")
    ids = expert_ids.T
    weight = down_weight[0]
    bf16, f32 = jnp.bfloat16, jnp.float32
    block = jax.ShapeDtypeStruct((2 * capacity, features // 2), bf16)
    outgoing = pl.pallas_call(
        functools.partial(dispatch_kernel, experts, capacity),
        out_shape=[block] * experts,
        in_specs=[VMEM] * 3,
        out_specs=[VMEM] * experts,
        compiler_params=pltpu.CompilerParams(vmem_limit_bytes=16 << 20),
        name="dispatch",
    )(ids, grad_out, history_grad)
    order = list(range(2, half)) + list(range(half, experts)) + [1]
    received = [outgoing[0]] + [None] * (experts - 1)
    for k in order:
        received[k] = lax.ppermute(
            outgoing[k], "expert", [(i, i ^ k) for i in range(experts)]
        )
    pair = jax.ShapeDtypeStruct((2 * capacity, units), bf16)
    scratch = [pltpu.VMEM((half * (capacity + 4), features // 2), bf16)] * 2
    params = pltpu.CompilerParams(vmem_limit_bytes=24 << 20)
    cost = pl.CostEstimate(
        flops=half * capacity * units * features * 2,
        bytes_accessed=units * features * 2,
        transcendentals=0,
    )
    *early, vector = pl.pallas_call(
        functools.partial(early_kernel, experts, capacity, half),
        out_shape=[pair] * (half // 2) + [jax.ShapeDtypeStruct((1, 128), f32)],
        in_specs=[VMEM] * (half + 5),
        out_specs=[VMEM] * (half // 2 + 1),
        scratch_shapes=scratch,
        compiler_params=params,
        cost_estimate=cost,
        name="early",
    )(*received[:half], weight, history_grad, history_hidden, ids, grad_out)
    *late, peaks = pl.pallas_call(
        functools.partial(late_kernel, experts, capacity, half),
        out_shape=[pair] * (half // 2) + [jax.ShapeDtypeStruct((devices, 128), f32)],
        in_specs=[VMEM] * (half + 4),
        out_specs=[VMEM] * (half // 2 + 1),
        scratch_shapes=scratch,
        compiler_params=params,
        cost_estimate=cost,
        name="late",
    )(*received[half:], weight, history_grad, history_hidden, vector)
    everyone = lax.all_to_all(peaks, ("dp", "expert"), 0, 0, tiled=True)
    hidden = pl.pallas_call(
        functools.partial(assemble_kernel, capacity),
        out_shape=jax.ShapeDtypeStruct((experts * capacity, units), bf16),
        in_specs=[VMEM] * half,
        out_specs=VMEM,
        compiler_params=pltpu.CompilerParams(vmem_limit_bytes=8 << 20),
        cost_estimate=pl.CostEstimate(
            flops=1 << 22, bytes_accessed=experts * capacity * units * 4, transcendentals=0
        ),
        name="assemble",
    )(*early, *late)
    new_history_grad, new_history_hidden = pl.pallas_call(
        functools.partial(finish_kernel, experts),
        out_shape=[jax.ShapeDtypeStruct(history_grad.shape, f32)] * 2,
        in_specs=[VMEM] * 3,
        out_specs=[VMEM] * 2,
        name="finish",
    )(everyone, history_grad, history_hidden)
    return hidden.reshape(1, 1, -1, units), new_history_grad, new_history_hidden


def general_device(grad_out, expert_ids, down_weight, history_grad, history_hidden):
    tok_rows = grad_out.shape[0]
    experts = history_grad.shape[1]
    slices = lax.axis_size("expert") // experts
    capacity = tok_rows * 9 // 32
    flat_ids = expert_ids.reshape(-1)
    onehot = (flat_ids[:, None] == jnp.arange(experts, dtype=jnp.int32)[None, :]).astype(jnp.int32)
    before = jnp.cumsum(onehot, axis=0) - onehot
    slot_index = jnp.sum(before * onehot, axis=1)
    target = flat_ids * capacity + slot_index
    matches = (jnp.arange(experts * capacity, dtype=jnp.int32)[:, None] == target[None, :]).astype(
        jnp.int32
    )
    dispatch = jnp.sum(matches.reshape(experts * capacity, tok_rows, 2), axis=2).astype(
        jnp.bfloat16
    )
    gathered = jnp.dot(dispatch, grad_out, preferred_element_type=jnp.float32)
    scale_in = 1.0 / jnp.max(history_grad, axis=0)
    scale_hidden = 1.0 / jnp.max(history_hidden, axis=0)
    quantized = jnp.clip(
        gathered.reshape(experts, capacity, -1) * scale_in[:, None, None], -1.0, 1.0
    ).astype(jnp.bfloat16)
    own_index = lax.axis_index("expert")
    own_expert = own_index // slices
    chosen = jnp.arange(experts, dtype=jnp.int32) == own_expert
    own_scale_in = jnp.sum(jnp.where(chosen, scale_in, 0.0))
    own_scale_hidden = jnp.sum(jnp.where(chosen, scale_hidden, 0.0))
    routed = jnp.max(onehot.reshape(tok_rows, 2, experts), axis=1) > 0
    row_peak = jnp.max(jnp.abs(grad_out.astype(jnp.float32)), axis=1)
    grad_peak = jnp.max(jnp.where(routed, row_peak[:, None], 0.0), axis=0)
    weight_block = down_weight[0]
    outgoing = jnp.repeat(quantized, slices, axis=0)
    received = lax.all_to_all(outgoing, "expert", split_axis=0, concat_axis=0, tiled=True)
    product = jnp.einsum("sic,uc->siu", received, weight_block, preferred_element_type=jnp.float32)
    hidden = product / own_scale_in
    hidden_peak = jnp.max(jnp.abs(hidden))
    hidden_vec = jnp.where(chosen, hidden_peak, 0.0)
    grad_amax, hidden_amax = lax.pmax((grad_peak, hidden_vec), ("dp", "expert"))
    scaled = jnp.clip(hidden * own_scale_hidden, -1.0, 1.0).astype(jnp.bfloat16)
    hidden_scaled = scaled.reshape(1, 1, -1, scaled.shape[2])
    new_history_grad = jnp.concatenate([history_grad[1:], grad_amax[None, :]], axis=0)
    new_history_hidden = jnp.concatenate([history_hidden[1:], hidden_amax[None, :]], axis=0)
    return (hidden_scaled, new_history_grad, new_history_hidden)


def per_device(grad_out, expert_ids, down_weight, history_grad, history_hidden):
    experts = history_grad.shape[1]
    whole_experts = lax.axis_size("expert") == experts
    paired = experts & (experts - 1) == 0 and experts >= 4
    device = fast_device if whole_experts and paired else general_device
    return device(grad_out, expert_ids, down_weight, history_grad, history_hidden)


def solution(mesh):
    in_specs = (
        P(("dp", "expert"), None),
        P(("dp", "expert"), None),
        P("expert", None, None),
        P(),
        P(),
    )
    out_specs = (P("dp", "expert", None, None), P(), P())
    return jax.shard_map(
        per_device, mesh=mesh, in_specs=in_specs, out_specs=out_specs, check_vma=False
    )
```

```python
import functools

import jax
import jax.numpy as jnp
from jax import lax
from jax.experimental import pallas as pl
from jax.experimental.pallas import tpu as pltpu
from jax.sharding import PartitionSpec as P


VMEM = pl.BlockSpec(memory_space=pltpu.VMEM)
ANY = pl.BlockSpec(memory_space=pl.ANY)


def choice_map(ids, order):
    return (ids[0:1, :] == order) | (ids[1:2, :] == order)


def pick(values, index):
    lanes = lax.broadcasted_iota(jnp.int32, values.shape, 1)
    return jnp.sum(jnp.where(lanes == index, values, 0.0), axis=1, keepdims=True)


def dispatch_kernel(experts, capacity, first, *refs):
    ids_hbm, grad_hbm, history_hbm = refs[:3]
    ids_ref, grad_ref, history_ref, sems = refs[-4:]
    out_refs = refs[-4 - experts // 2 : -4]
    copies = [
        pltpu.make_async_copy(source, target, sems.at[i])
        for i, (source, target) in enumerate(
            ((ids_hbm, ids_ref), (history_hbm, history_ref), (grad_hbm, grad_ref))
        )
    ]
    for copy in copies:
        copy.start()
    tokens, features = grad_ref.shape
    half = features // 2
    base = capacity // 8 * 8
    rest = capacity - base
    me = lax.axis_index("expert")
    order = lax.broadcasted_iota(jnp.int32, (experts, tokens), 0) ^ me
    before = (
        lax.broadcasted_iota(jnp.int32, (tokens, tokens), 0)
        < lax.broadcasted_iota(jnp.int32, (tokens, tokens), 1)
    )
    rows = lax.broadcasted_iota(jnp.int32, (2 * capacity, tokens), 0)
    low_slot = jnp.where(rows < capacity, rows, -1)
    high_slot = jnp.where(
        rows < capacity, -1, jnp.where(rows < capacity + rest, rows - capacity + base, rows - capacity - rest)
    )
    copies[0].wait()
    named = choice_map(ids_ref[...], order)
    slot = jnp.dot(
        jnp.where(named, 1.0, 0.0).astype(jnp.bfloat16),
        jnp.where(before, 1.0, 0.0).astype(jnp.bfloat16),
        preferred_element_type=jnp.float32,
    ).astype(jnp.int32)
    slot = jnp.where(named, slot, -2)
    copies[1].wait()
    scale = 1.0 / jnp.max(history_ref[...], axis=0, keepdims=True)
    copies[2].wait()
    stacked = jnp.concatenate([grad_ref[:, :half], grad_ref[:, half:]], axis=0)
    for i, out_ref in enumerate(out_refs):
        k = first + i
        mine = slot[k : k + 1, :]
        low = jnp.where(mine == low_slot, 1.0, 0.0)
        high = jnp.where(mine == high_slot, 1.0, 0.0)
        select = jnp.concatenate([low, high], axis=1).astype(jnp.bfloat16)
        rowsum = jnp.dot(select, stacked, preferred_element_type=jnp.float32)
        factor = pick(scale, me ^ k)
        out_ref[...] = jnp.clip(rowsum * factor, -1.0, 1.0).astype(jnp.bfloat16)


def gather_rows(blocks, capacity, rows_ref):
    base = capacity // 8 * 8
    rest = capacity - base
    half = rows_ref.shape[1] // 2
    step = base + 8
    keep = lax.broadcasted_iota(jnp.int32, (8, half), 0) < rest
    for i, block in enumerate(blocks):
        at = i * step
        rows_ref[at : at + base, :half] = block[0:base, :]
        rows_ref[at : at + base, half:] = block[base + 8 :, :]
        mixed = block[base : base + 8, :].astype(jnp.float32)
        turned = jnp.concatenate([mixed[rest:], mixed[:rest]], axis=0)
        rows_ref[at + base : at + step, :half] = jnp.where(keep, mixed, 0.0).astype(jnp.bfloat16)
        rows_ref[at + base : at + step, half:] = jnp.where(keep, turned, 0.0).astype(jnp.bfloat16)


def largest(product, restore):
    peak = jnp.max(jnp.abs(product), axis=0, keepdims=True)
    return jnp.max(peak, axis=1, keepdims=True) * restore


def prepare_kernel(experts, weight_ref, ids_ref, grad_ref, turned_ref, vector_ref):
    turned_ref[...] = weight_ref[...].T
    tokens = grad_ref.shape[0]
    order = lax.broadcasted_iota(jnp.int32, (experts, tokens), 0)
    named = choice_map(ids_ref[...], order)
    row_peak = jnp.max(jnp.abs(grad_ref[...].astype(jnp.float32)), axis=1, keepdims=True)
    row_peak = jnp.broadcast_to(row_peak, (tokens, tokens)).T[0:1, :]
    grad_peak = jnp.max(jnp.where(named, row_peak, 0.0), axis=1, keepdims=True)
    lanes = lax.broadcasted_iota(jnp.int32, (experts, 128), 1)
    spread = jnp.where(
        lanes == lax.broadcasted_iota(jnp.int32, (experts, 128), 0), grad_peak, 0.0
    )
    vector_ref[...] = jnp.max(spread, axis=0, keepdims=True)


def project_kernel(experts, capacity, count, *refs):
    blocks = refs[:count]
    turned_ref, history_grad_ref, vector_ref, product_ref, peaks_ref, rows_ref = refs[count:]
    me = lax.axis_index("expert")
    gather_rows(blocks, capacity, rows_ref)
    product = jnp.dot(rows_ref[...], turned_ref[...], preferred_element_type=jnp.float32)
    product_ref[...] = product
    scale_in = pick(1.0 / jnp.max(history_grad_ref[...], axis=0, keepdims=True), me)
    peak = largest(product, 1.0 / scale_in)
    lane = lax.broadcasted_iota(jnp.int32, (1, 128), 1)
    vector = jnp.maximum(vector_ref[...], jnp.where(lane == experts + me, peak, 0.0))
    peaks_ref[...] = jnp.broadcast_to(vector, peaks_ref.shape)


def assemble_kernel(capacity, early_ref, late_ref, history_grad_ref, history_hidden_ref, out_ref):
    me = lax.axis_index("expert")
    chip = me // 2
    first_core = (me & 1) == 0
    step = capacity // 8 * 8 + 8
    scale_in = pick(1.0 / jnp.max(history_grad_ref[...], axis=0, keepdims=True), me)
    scale_hidden = pick(1.0 / jnp.max(history_hidden_ref[...], axis=0, keepdims=True), me)
    restore = 1.0 / scale_in
    pairs = early_ref.shape[0] // step // 2
    for j in range(2 * pairs):
        ref, at = (early_ref, j) if j < pairs else (late_ref, j - pairs)
        at = 2 * at * step
        a, b = ref[at : at + capacity, :], ref[at + step : at + step + capacity, :]
        both = jnp.concatenate([jnp.where(first_core, a, b), jnp.where(first_core, b, a)], axis=0)
        both = jnp.clip(both * restore * scale_hidden, -1.0, 1.0).astype(jnp.bfloat16)
        start = pl.multiple_of((chip ^ j) * 2 * capacity, 8)
        out_ref[pl.ds(start, 2 * capacity), :] = both


def sending_order(experts):
    half = experts // 2
    return [
        *range(half, half + half // 2), *range(2, half), 1, *range(half + half // 2, experts)
    ]


def fast_device(grad_out, expert_ids, down_weight, history_grad, history_hidden):
    tokens, features = grad_out.shape
    experts = history_grad.shape[1]
    capacity = tokens * 9 // 32
    units = down_weight.shape[1]
    half = experts // 2
    devices = lax.axis_size("dp") * lax.axis_size("expert")
    ids = expert_ids.T
    weight = down_weight[0]
    bf16, f32 = jnp.bfloat16, jnp.float32
    block = jax.ShapeDtypeStruct((2 * capacity, features // 2), bf16)

    def dispatch(first, after):
        return pl.pallas_call(
            functools.partial(dispatch_kernel, experts, capacity, first),
            out_shape=[block] * half,
            in_specs=[pl.BlockSpec(memory_space=pltpu.HBM)] * 3 + [ANY] * len(after),
            out_specs=[VMEM] * half,
            scratch_shapes=[
                pltpu.VMEM(ids.shape, jnp.int32),
                pltpu.VMEM(grad_out.shape, bf16),
                pltpu.VMEM(history_grad.shape, f32),
                pltpu.SemaphoreType.DMA((3,)),
            ],
            compiler_params=pltpu.CompilerParams(vmem_limit_bytes=16 << 20),
            cost_estimate=pl.CostEstimate(
                flops=1 << 28, bytes_accessed=grad_out.size * 4, transcendentals=0
            ),
        )(*(pltpu.with_memory_space_constraint(x, pltpu.HBM) for x in (ids, grad_out, history_grad)), *after)

    far = dispatch(half, ())
    near = dispatch(0, (far[0],))
    received = [near[0]] + [None] * (experts - 1)
    for k in sending_order(experts):
        received[k] = lax.ppermute((near + far)[k], "expert", [(i, i ^ k) for i in range(experts)])
    rows = half * (capacity // 8 * 8 + 8)
    product = jax.ShapeDtypeStruct((rows, units), f32)
    scratch = [pltpu.VMEM((rows, features), bf16)]
    params = pltpu.CompilerParams(vmem_limit_bytes=24 << 20)
    cost = pl.CostEstimate(
        flops=rows * units * features * 2, bytes_accessed=units * features * 2, transcendentals=0
    )
    turned, vector = pl.pallas_call(
        functools.partial(prepare_kernel, experts),
        out_shape=[
            jax.ShapeDtypeStruct((features, units), bf16),
            jax.ShapeDtypeStruct((1, 128), f32),
        ],
        in_specs=[VMEM] * 3,
        out_specs=[VMEM] * 2,
        compiler_params=params,
        cost_estimate=cost,
        name="prepare",
    )(weight, ids, grad_out)

    def project(blocks, vector, copies):
        return pl.pallas_call(
            functools.partial(project_kernel, experts, capacity, len(blocks)),
            out_shape=[product, jax.ShapeDtypeStruct((copies, 128), f32)],
            in_specs=[VMEM] * (len(blocks) + 3),
            out_specs=[VMEM] * 2,
            scratch_shapes=scratch,
            compiler_params=params,
            cost_estimate=cost,
        )(*blocks, turned, history_grad, vector)

    early, vector = project(received[:half], vector, 1)
    late, peaks = project(received[half:], vector, devices)
    everyone = lax.all_to_all(peaks, ("dp", "expert"), 0, 0, tiled=True)
    hidden = pl.pallas_call(
        functools.partial(assemble_kernel, capacity),
        out_shape=jax.ShapeDtypeStruct((experts * capacity, units), bf16),
        in_specs=[VMEM] * 4,
        out_specs=VMEM,
        compiler_params=pltpu.CompilerParams(vmem_limit_bytes=8 << 20),
        cost_estimate=pl.CostEstimate(
            flops=1 << 22, bytes_accessed=experts * capacity * units * 4, transcendentals=0
        ),
        name="assemble",
    )(early, late, history_grad, history_hidden)
    top = jnp.max(everyone, axis=0)
    new_history_grad = jnp.concatenate([history_grad[1:], top[None, :experts]], axis=0)
    new_history_hidden = jnp.concatenate(
        [history_hidden[1:], top[None, experts : 2 * experts]], axis=0
    )
    return hidden.reshape(1, 1, -1, units), new_history_grad, new_history_hidden


def general_device(grad_out, expert_ids, down_weight, history_grad, history_hidden):
    tok_rows = grad_out.shape[0]
    experts = history_grad.shape[1]
    slices = lax.axis_size("expert") // experts
    capacity = tok_rows * 9 // 32
    flat_ids = expert_ids.reshape(-1)
    onehot = (flat_ids[:, None] == jnp.arange(experts, dtype=jnp.int32)[None, :]).astype(jnp.int32)
    before = jnp.cumsum(onehot, axis=0) - onehot
    slot_index = jnp.sum(before * onehot, axis=1)
    target = flat_ids * capacity + slot_index
    matches = (jnp.arange(experts * capacity, dtype=jnp.int32)[:, None] == target[None, :]).astype(
        jnp.int32
    )
    dispatch = jnp.sum(matches.reshape(experts * capacity, tok_rows, 2), axis=2).astype(
        jnp.bfloat16
    )
    gathered = jnp.dot(dispatch, grad_out, preferred_element_type=jnp.float32)
    scale_in = 1.0 / jnp.max(history_grad, axis=0)
    scale_hidden = 1.0 / jnp.max(history_hidden, axis=0)
    quantized = jnp.clip(
        gathered.reshape(experts, capacity, -1) * scale_in[:, None, None], -1.0, 1.0
    ).astype(jnp.bfloat16)
    own_index = lax.axis_index("expert")
    own_expert = own_index // slices
    chosen = jnp.arange(experts, dtype=jnp.int32) == own_expert
    own_scale_in = jnp.sum(jnp.where(chosen, scale_in, 0.0))
    own_scale_hidden = jnp.sum(jnp.where(chosen, scale_hidden, 0.0))
    routed = jnp.max(onehot.reshape(tok_rows, 2, experts), axis=1) > 0
    row_peak = jnp.max(jnp.abs(grad_out.astype(jnp.float32)), axis=1)
    grad_peak = jnp.max(jnp.where(routed, row_peak[:, None], 0.0), axis=0)
    weight_block = down_weight[0]
    outgoing = jnp.repeat(quantized, slices, axis=0)
    received = lax.all_to_all(outgoing, "expert", split_axis=0, concat_axis=0, tiled=True)
    product = jnp.einsum("sic,uc->siu", received, weight_block, preferred_element_type=jnp.float32)
    hidden = product / own_scale_in
    hidden_peak = jnp.max(jnp.abs(hidden))
    hidden_vec = jnp.where(chosen, hidden_peak, 0.0)
    grad_amax, hidden_amax = lax.pmax((grad_peak, hidden_vec), ("dp", "expert"))
    scaled = jnp.clip(hidden * own_scale_hidden, -1.0, 1.0).astype(jnp.bfloat16)
    hidden_scaled = scaled.reshape(1, 1, -1, scaled.shape[2])
    new_history_grad = jnp.concatenate([history_grad[1:], grad_amax[None, :]], axis=0)
    new_history_hidden = jnp.concatenate([history_hidden[1:], hidden_amax[None, :]], axis=0)
    return (hidden_scaled, new_history_grad, new_history_hidden)


def is_fast(expert_devices, experts, capacity):
    power = experts & (experts - 1) == 0 and experts >= 4
    return expert_devices == experts and power and capacity % 8 == 4


def per_device(grad_out, expert_ids, down_weight, history_grad, history_hidden):
    experts = history_grad.shape[1]
    capacity = grad_out.shape[0] * 9 // 32
    fast = is_fast(lax.axis_size("expert"), experts, capacity)
    device = fast_device if fast else general_device
    return device(grad_out, expert_ids, down_weight, history_grad, history_hidden)


def solution(mesh):
    in_specs = (
        P(("dp", "expert"), None),
        P(("dp", "expert"), None),
        P("expert", None, None),
        P(),
        P(),
    )
    out_specs = (P("dp", "expert", None, None), P(), P())
    return jax.shard_map(
        per_device, mesh=mesh, in_specs=in_specs, out_specs=out_specs, check_vma=False
    )
```
